32 devices in a mesh: data: 32 (over z, y, x, core).
Axes of the slice: x: 2, y: 2, z: 4, core: 2. Of those that a mesh axis runs over, the one named last changes fastest.
Arguments:
- tok_ids: int32 [32768], P('data')
- grad_out: bfloat16 [32768, 1024], P('data')
- n_real: int32 [32], P('data')
- embed_table: bfloat16 [50265, 1024], replicated
- w_in: bfloat16 [1024, 4096], replicated
- w_out: bfloat16 [4096, 1024], replicated
Outputs:
- output 1: float32 [50265, 1024], replicated
- output 2: float32 [1024, 4096], replicated
- output 3: float32 [4096, 1024], replicated
All inputs are finite; a program needn't handle non-finite values.
Results may differ from the reference program's by a relative error of at most 0.00849531.
Values are sent between devices in bfloat16 or wider.
A program may use at most 1.5 GiB of HBM per device.

```python
import math
import jax
import jax.numpy as jnp
from jax import lax

NUM_DEV = 32
TOKENS = 1024
VOCAB = 50265
DIM = 1024
FFN = 4096

UNIQ_IDS = TOKENS // 4
SHARED_IDS = UNIQ_IDS // 2
GELU_A = 0.044715
GELU_C = math.sqrt(2.0 / math.pi)


def draw_ids(rng_key):
    k_perm, k_dev = jax.random.split(rng_key)
    vocab_perm = jax.random.permutation(k_perm, VOCAB)
    shared_ids = vocab_perm[:SHARED_IDS]
    other_ids = vocab_perm[SHARED_IDS:]

    def one_device(dev_key):
        k_own, k_order, k_fill = jax.random.split(dev_key, 3)
        own_pick = jax.random.permutation(k_own, VOCAB - SHARED_IDS)[:UNIQ_IDS - SHARED_IDS]
        distinct = jnp.concatenate([shared_ids, other_ids[own_pick]])
        distinct = jax.random.permutation(k_order, distinct)
        filler = distinct[jax.random.randint(k_fill, (TOKENS - UNIQ_IDS,), 0, UNIQ_IDS)]
        return jnp.concatenate([distinct, filler])

    per_dev = jax.vmap(one_device)(jax.random.split(k_dev, NUM_DEV))
    return per_dev.reshape(NUM_DEV * TOKENS).astype(jnp.int32)


def draw_lengths(rng_key):
    k_len, k_pos = jax.random.split(rng_key)
    lengths = jax.random.randint(k_len, (NUM_DEV,), TOKENS // 4, TOKENS + 1)
    dev_order = jax.random.permutation(k_pos, NUM_DEV)
    lengths = lengths.at[dev_order[0]].set(TOKENS).at[dev_order[1]].set(TOKENS // 4)
    return lengths.astype(jnp.int32)


def setup_inputs(seed: int = 0) -> dict:
    root_key = jax.random.key(seed)
    k_ids, k_len, k_dy, k_tab, k_in, k_out = jax.random.split(root_key, 6)
    grad_out = jax.random.normal(k_dy, (NUM_DEV * TOKENS, DIM), jnp.float32) * NUM_DEV ** -0.5
    embed_table = jax.random.normal(k_tab, (VOCAB, DIM), jnp.float32)
    w_in = jax.random.normal(k_in, (DIM, FFN), jnp.float32) * DIM ** -0.5
    w_out = jax.random.normal(k_out, (FFN, DIM), jnp.float32) * FFN ** -0.5
    return {
        'tok_ids': draw_ids(k_ids),
        'grad_out': grad_out.astype(jnp.bfloat16),
        'n_real': draw_lengths(k_len),
        'embed_table': embed_table.astype(jnp.bfloat16),
        'w_in': w_in.astype(jnp.bfloat16),
        'w_out': w_out.astype(jnp.bfloat16),
    }


def gelu_and_slope(pre_act):
    z_val = pre_act.astype(jnp.float32)
    tanh_val = jnp.tanh(GELU_C * (z_val + GELU_A * z_val * z_val * z_val))
    act_val = 0.5 * z_val * (1.0 + tanh_val)
    slope_val = 0.5 * (1.0 + tanh_val) + 0.5 * z_val * (1.0 - tanh_val * tanh_val) * GELU_C * (1.0 + 3.0 * GELU_A * z_val * z_val)
    return act_val, slope_val


def device_grads(ids_one, dy_one, n_one, embed_table, w_in, w_out):
    x_rows = jnp.take(embed_table, ids_one, axis=0)
    keep_mask = (jnp.arange(ids_one.shape[0]) < n_one)[:, None]
    dy_kept = jnp.where(keep_mask, dy_one, jnp.zeros_like(dy_one))
    pre_act = jnp.dot(x_rows, w_in, preferred_element_type=jnp.float32).astype(jnp.bfloat16)
    act_val, slope_val = gelu_and_slope(pre_act)
    act_bf16 = act_val.astype(jnp.bfloat16)
    part_out = jnp.dot(act_bf16.T, dy_kept, preferred_element_type=jnp.float32)
    grad_act = jnp.dot(dy_kept, w_out.T, preferred_element_type=jnp.float32).astype(jnp.bfloat16)
    grad_pre = (grad_act.astype(jnp.float32) * slope_val).astype(jnp.bfloat16)
    part_in = jnp.dot(x_rows.T, grad_pre, preferred_element_type=jnp.float32)
    grad_x = (dy_kept.astype(jnp.float32) + jnp.dot(grad_pre, w_in.T, preferred_element_type=jnp.float32)).astype(jnp.bfloat16)
    return grad_x, part_in, part_out


def reference(tok_ids, grad_out, n_real, embed_table, w_in, w_out):
    ids_dev = tok_ids.reshape(NUM_DEV, TOKENS)
    dy_dev = grad_out.reshape(NUM_DEV, TOKENS, DIM)

    def body(carry_acc, per_dev):
        acc_in, acc_out = carry_acc
        ids_one, dy_one, n_one = per_dev
        grad_x, part_in, part_out = device_grads(ids_one, dy_one, n_one, embed_table, w_in, w_out)
        return (acc_in + part_in, acc_out + part_out), grad_x

    init_acc = (jnp.zeros((DIM, FFN), jnp.float32), jnp.zeros((FFN, DIM), jnp.float32))
    (grad_w_in, grad_w_out), grad_x = lax.scan(body, init_acc, (ids_dev, dy_dev, n_real))
    flat_rows = grad_x.reshape(NUM_DEV * TOKENS, DIM).astype(jnp.float32)
    grad_table = jax.ops.segment_sum(flat_rows, tok_ids, num_segments=VOCAB)
    return grad_table, grad_w_in, grad_w_out
```

```python
import math
import jax
import jax.numpy as jnp
from jax import lax
from jax.experimental import pallas as pl
from jax.experimental.pallas import tpu as pltpu
from jax.sharding import PartitionSpec as P


GELU_A = 0.044715
GELU_C = math.sqrt(2.0 / math.pi)
F32 = jnp.float32
BF16 = jnp.bfloat16

TOK = 1024
DIM = 1024
FFN = 4096
VOCAB = 50265
UNIQ = 256
BLOCK = UNIQ + 8
NDEV = 32
TABLE_ROWS = 1024
UNROLL = 8
TABLE_STEPS = -(-VOCAB // TABLE_ROWS)


def device_index(z, y, x, c):
    return ((z * 2 + y) * 2 + x) * 2 + c


COORDS = [(z, y, x, c) for z in range(4) for y in range(2) for x in range(2) for c in range(2)]
PAIRS_X = [(device_index(z, y, x, c), device_index(z, y, 1 - x, c)) for z, y, x, c in COORDS]
PAIRS_Y = [(device_index(z, y, x, c), device_index(z, 1 - y, x, c)) for z, y, x, c in COORDS]
PAIRS_C = [(device_index(z, y, x, c), device_index(z, y, x, 1 - c)) for z, y, x, c in COORDS]


def pairs_up(senders):
    return [(device_index(z, y, x, c), device_index(z + 1, y, x, c)) for z, y, x, c in COORDS if z in senders]


def pairs_down(senders):
    return [(device_index(z, y, x, c), device_index(z - 1, y, x, c)) for z, y, x, c in COORDS if z in senders]


def send(arr, pairs):
    return lax.ppermute(arr, 'data', pairs)


def pick_at(arr, i, axis):
    return lax.dynamic_index_in_dim(arr, i, axis=axis, keepdims=False)


def scatter_sum(part, x, y, z):
    rows, width = part.shape
    k = rows // 32
    part = part.reshape(2, 2, 4, 2, k, width)
    ox, oy = 1 - x, 1 - y

    def cut(arr, i, j, half):
        sizes = (arr.shape[0] if i is None else 1, arr.shape[1] if j is None else 1, 4, 1, k, width)
        return lax.dynamic_slice(arr, (0 if i is None else i, 0 if j is None else j, 0, half, 0, 0), sizes)

    away_a = cut(part, ox, None, 0)
    away_b = cut(part, None, oy, 1)
    got_a = send(away_a, PAIRS_X)
    got_b = send(away_b, PAIRS_Y)
    away_a = cut(part, x, oy, 0) + cut(got_a, None, oy, 0)
    away_b = cut(part, ox, y, 1) + cut(got_b, ox, None, 0)
    last_a = send(away_a, PAIRS_Y)
    last_b = send(away_b, PAIRS_X)
    sum_a = cut(part, x, y, 0) + cut(got_a, None, y, 0) + last_a
    sum_b = cut(part, x, y, 1) + cut(got_b, x, None, 0) + last_b
    col = jnp.concatenate([sum_a, sum_b], axis=3).reshape(4, 2, k, width)

    def shard(i):
        return pick_at(col, jnp.clip(i, 0, 3), 0)

    up = send(shard(z + 3), pairs_up([0]))
    down = send(shard(z - 3), pairs_down([3]))
    up = send(shard(z + 2) + up, pairs_up([0, 1]))
    down = send(shard(z - 2) + down, pairs_down([3, 2]))
    up = send(shard(z + 1) + up, pairs_up([0, 1, 2]))
    down = send(shard(z - 1) + down, pairs_down([3, 2, 1]))
    return shard(z) + up + down


def gather_column(block, z):
    up, down = [block], [block]
    for step in range(1, 4):
        up.append(send(up[-1], pairs_up(range(step - 1, 3))))
        down.append(send(down[-1], pairs_down(range(1, 5 - step))))
    seven = jnp.stack([up[3], up[2], up[1], block, down[1], down[2], down[3]])
    return lax.dynamic_slice_in_dim(seven, 3 - z, 4, axis=0)


def gather_plane(col):
    gx = send(col, PAIRS_X)
    gy = send(col, PAIRS_Y)
    low = send(gy[:2], PAIRS_X)
    high = send(gx[2:], PAIRS_Y)
    return [col, gx, gy, low, high]


def cross(pieces):
    return [send(p, PAIRS_C) for p in pieces]


def blank(shape):
    return pl.pallas_call(lambda ref: None, out_shape=jax.ShapeDtypeStruct(shape, F32), out_specs=pl.BlockSpec(memory_space=pl.ANY), name='blank')()


def gather_weight(shard, x, y, z, c):
    width = shard.shape[-1]
    k = shard.shape[1]
    pieces = gather_plane(gather_column(shard, z))
    out = blank((64 * k, width))
    ox, oy = 1 - x, 1 - y
    places = ((x, y, 0), (ox, y, 0), (x, oy, 0), (ox, oy, 0), (ox, oy, 2))
    for lane, parts in ((c, pieces), (1 - c, cross(pieces))):
        for p, (i, j, first) in zip(parts, places):
            out = lax.dynamic_update_slice_in_dim(out, p.reshape(-1, width), lane * 32 * k + ((i * 2 + j) * 8 + first * 2) * k, axis=0)
    return out


def table_kernel(start_ref, entry_ref, row_ref, *refs):
    pieces, (out_ref, rows, sem) = refs[:-3], refs[-3:]
    step = pl.program_id(0)

    @pl.when(step == 0)
    def _():
        base = 0
        copies = []
        for piece in pieces:
            for j in range(piece.shape[0]):
                copies.append(pltpu.make_async_copy(piece.at[j], rows.at[pl.ds(base, BLOCK)], sem.at[len(copies)]))
                base += BLOCK
        for cp in copies:
            cp.start()
        for cp in copies:
            cp.wait()

    out_ref[...] = jnp.zeros_like(out_ref)

    def add_row(i, acc):
        entry = entry_ref[i]
        r = entry & (TABLE_ROWS - 1)
        acc = rows[pl.ds(row_ref[i], 1), :] + jnp.where(entry >= TABLE_ROWS, acc, 0.0)
        out_ref[pl.ds(r, 1), :] = acc
        return acc

    def add_rows(g, acc):
        for k in range(UNROLL):
            acc = add_row(first + g * UNROLL + k, acc)
        return acc

    first, last = start_ref[step], start_ref[step + 1]
    whole = (last - first) // UNROLL
    acc = lax.fori_loop(0, whole, add_rows, jnp.zeros((1, DIM), F32))
    lax.fori_loop(first + whole * UNROLL, last, add_row, acc)


def build_table(pieces):
    keys = jnp.concatenate([p[:, UNIQ, :UNIQ].reshape(-1) for p in pieces]).astype(jnp.int32)
    n = keys.shape[0]
    place = jnp.arange(n, dtype=jnp.int32)
    place = (place // UNIQ) * BLOCK + place % UNIQ
    keys, place = lax.sort((keys, place), num_keys=1)
    ids = keys // NDEV
    same = jnp.concatenate([jnp.zeros((1,), bool), ids[1:] == ids[:-1]])
    entry = ids % TABLE_ROWS + jnp.where(same, TABLE_ROWS, 0)
    bounds = jnp.arange(TABLE_STEPS + 1, dtype=jnp.int32) * TABLE_ROWS
    starts = jnp.sum(ids[None, :] < bounds[:, None], axis=1, dtype=jnp.int32)
    return pl.pallas_call(
        table_kernel,
        out_shape=jax.ShapeDtypeStruct((VOCAB, DIM), F32),
        grid_spec=pltpu.PrefetchScalarGridSpec(
            num_scalar_prefetch=3,
            grid=(TABLE_STEPS,),
            in_specs=[pl.BlockSpec(memory_space=pl.ANY)] * len(pieces),
            out_specs=pl.BlockSpec((TABLE_ROWS, DIM), lambda i, *_: (i, 0)),
            scratch_shapes=[
                pltpu.VMEM((NDEV * BLOCK, DIM), F32),
                pltpu.SemaphoreType.DMA((NDEV,)),
            ],
        ),
        compiler_params=pltpu.CompilerParams(vmem_limit_bytes=56 * 1024 * 1024),
        cost_estimate=pl.CostEstimate(flops=80_000_000_000, bytes_accessed=240_000_000, transcendentals=0),
        name='table_build',
    )(starts, entry, place, *pieces)


def dot(a, b, dims):
    return lax.dot_general(a, b, (dims, ((), ())), preferred_element_type=F32)


def solution(mesh):
    def per_device(tok_ids, grad_out, n_real, embed_table, w_in, w_out):
        dev = lax.axis_index('data')
        c, x, y, z = dev % 2, (dev // 2) % 2, (dev // 4) % 2, dev // 8

        pos = jnp.arange(TOK, dtype=jnp.int32)
        seen = (tok_ids[:, None] == tok_ids[None, :]) & (pos[None, :] < pos[:, None])
        first = ~jnp.any(seen, axis=1)
        rank = jnp.sum((tok_ids[None, :] < tok_ids[:, None]) & first[None, :], axis=1, dtype=jnp.int32)
        slot = jnp.arange(UNIQ, dtype=jnp.int32)
        hit = rank[None, :] == slot[:, None]
        uniq = jnp.sum(jnp.where(hit & first[None, :], tok_ids[None, :], 0), axis=1, dtype=jnp.int32)
        pick = (rank[:, None] == slot[None, :]).astype(BF16)
        pick_t = hit.astype(BF16)

        x_uniq = jnp.take(embed_table, uniq, axis=0)
        z_uniq = dot(x_uniq, w_in, ((1,), (0,))).astype(BF16)
        zu = z_uniq.astype(F32)
        h_uniq = (0.5 * zu * (1.0 + jnp.tanh(GELU_C * (zu + GELU_A * zu * zu * zu)))).astype(BF16)

        dy = jnp.where((pos < n_real[0])[:, None], grad_out, jnp.zeros_like(grad_out))

        def act_half(lane):
            return dot(pick, lax.dynamic_slice_in_dim(h_uniq, lane * (FFN // 2), FFN // 2, axis=1), ((1,), (0,))).astype(BF16)

        out_far = dot(act_half(1 - c), dy, ((0,), (0,)))
        out_away = send(out_far, PAIRS_C)
        out_own = dot(act_half(c), dy, ((0,), (0,))) + out_away

        grad_act = dot(dy, w_out, ((1,), (1,))).astype(BF16)
        z_val = dot(pick, z_uniq, ((1,), (0,))).astype(BF16).astype(F32)
        tanh_val = jnp.tanh(GELU_C * (z_val + GELU_A * z_val * z_val * z_val))
        slope = 0.5 * (1.0 + tanh_val) + 0.5 * z_val * (1.0 - tanh_val * tanh_val) * GELU_C * (1.0 + 3.0 * GELU_A * z_val * z_val)
        grad_pre = (grad_act.astype(F32) * slope).astype(BF16)

        def x_half(lane):
            return dot(pick, lax.dynamic_slice_in_dim(x_uniq, lane * (DIM // 2), DIM // 2, axis=1), ((1,), (0,))).astype(BF16)

        in_far = dot(x_half(1 - c), grad_pre, ((0,), (0,)))
        in_away = send(in_far, PAIRS_C)
        in_own = dot(x_half(c), grad_pre, ((0,), (0,))) + in_away

        grad_x = (dy.astype(F32) + dot(grad_pre, w_in, ((1,), (1,)))).astype(BF16)
        summed = dot(pick_t, grad_x, ((1,), (0,)))
        keys = (uniq * NDEV + dev).astype(F32)
        block = jnp.concatenate([summed, jnp.pad(keys[None, :], ((0, 7), (0, DIM - UNIQ)))], axis=0)

        shard_out = scatter_sum(out_own, x, y, z)
        shard_in = scatter_sum(in_own, x, y, z)

        parts = gather_plane(gather_column(block, z))
        grad_table = build_table(parts + cross(parts))

        grad_w_out = gather_weight(shard_out, x, y, z, c)
        grad_w_in = gather_weight(shard_in, x, y, z, c)
        return grad_table, grad_w_in, grad_w_out

    return jax.shard_map(per_device, mesh=mesh, in_specs=(P('data'), P('data', None), P('data'), P(), P(), P()), out_specs=(P(), P(), P()), check_vma=False)
```
